256 devices in a mesh: px: 8 (over z_hi, x), py: 32 (over y, z_lo, core).
Axes of the slice: x: 4, y: 4, z: 8 (z_hi: 2, z_lo: 4; z = z_hi * 4 + z_lo), core: 2. Of those that a mesh axis runs over, the one named last changes fastest.
Arguments:
- populations: float32 [19, 2, 2048, 2048], P(None, None, ('py', 'px')), may hold values from 0.02 to 0.12
- pore: int32 [2, 2048, 2048], P(None, ('py', 'px')), may hold values 0 or 1
Outputs:
- flow: float32 [19, 2, 2048, 2048], P(None, None, 'py', 'px')
The draws below stay inside these ranges and needn't reach their ends.
All inputs are finite; a program needn't handle non-finite values. No bound on the sum of `pore` on one device may be relied on, other than what follows from the above.
Results may differ from the reference program's by a relative error of at most 0.0001.
Values sent between devices are 32-bit elements; how exact they have to be, the bound alone decides.
A program may use at most 128 MiB of HBM per device.

```python
import jax
import jax.numpy as jnp

Q = 19
NZ = 2
STEPS = 2
NX = 2048
NY = 2048


def with_ends(values, key, least, largest):
    extent = values.shape
    index_at = [jax.random.randint(jax.random.fold_in(key, axis), (), 0, extent[axis]) for axis in range(len(extent))]
    values = values.at[tuple(index_at)].set(least)
    longest = extent.index(max(extent))
    index_at[longest] = (index_at[longest] + 1) % extent[longest]
    return values.at[tuple(index_at)].set(largest)


def block_levels(rng, dims, shards, low, top_value):
    factor_of = 1.0
    for dim, blocks in shards:
        heights = jax.random.uniform(jax.random.fold_in(jax.random.fold_in(rng, 6), dim), (blocks,), jnp.float32, low / len(shards), top_value / len(shards))
        factor_of = factor_of * jnp.repeat(jnp.exp(heights), dims[dim] // blocks).reshape((-1,) + (1,) * (len(dims) - 1 - dim))
    return factor_of


def setup_inputs(seed: int = 0) -> dict:
    streams_of = jax.random.split(jax.random.key(seed), 3)
    populations = jnp.clip(0.02 + 0.09999999776482582 * jax.random.uniform(streams_of[0], (Q, NZ, NY, NX), jnp.float32) ** block_levels(streams_of[0], (Q, NZ, NY, NX), ((2, 256),), -0.2, 0.2), 0.02, 0.12)
    pore = with_ends((jax.random.randint(streams_of[1], (NZ, NY, NX), 0, 4) < 3).astype(jnp.int32), jax.random.fold_in(streams_of[1], 1), 0, 1)
    return {"populations": populations, "pore": pore}


lattice_velocity = [(0, 0, 0), (1, 0, 0), (-1, 0, 0), (0, 1, 0), (0, -1, 0), (0, 0, 1), (0, 0, -1),
                    (1, 1, 0), (-1, -1, 0), (1, -1, 0), (-1, 1, 0), (1, 0, 1), (-1, 0, -1), (1, 0, -1),
                    (-1, 0, 1), (0, 1, 1), (0, -1, -1), (0, 1, -1), (0, -1, 1)]
lattice_weights = [1.0 / 3.0] + [1.0 / 18.0] * 6 + [1.0 / 36.0] * 12
opposite = [0, 2, 1, 4, 3, 6, 5, 8, 7, 10, 9, 12, 11, 14, 13, 16, 15, 18, 17]
relax_time = 0.8
body_force = 0.005


def moment(fields, column):
    total = jnp.zeros_like(fields[0])
    for slot in range(len(lattice_velocity)):
        vector = lattice_velocity[slot]
        if vector[column] != 0:
            total = total + float(vector[column]) * fields[slot]
    return total


def collide(fields, fluid):
    density = jnp.where(fluid > 0.5, jnp.sum(fields, axis=0), 1.0)
    vel_first = moment(fields, 0) / density
    vel_second = moment(fields, 1) / density
    vel_third = moment(fields, 2) / density + relax_time * body_force
    speed = vel_first * vel_first + vel_second * vel_second + vel_third * vel_third
    result = []
    for slot in range(len(lattice_velocity)):
        vector = lattice_velocity[slot]
        along = vector[0] * vel_first + vector[1] * vel_second + vector[2] * vel_third
        equil = lattice_weights[slot] * density * (1.0 + 3.0 * along + 4.5 * along * along - 1.5 * speed)
        result.append(fields[slot] - (fields[slot] - equil) / relax_time)
    return jnp.stack(result) * fluid[None]


def reference(populations, pore):
    fluid = pore.astype(jnp.float32)
    fields = populations
    for step in range(STEPS):
        post = collide(fields, fluid)
        result = []
        for slot in range(len(lattice_velocity)):
            vector = lattice_velocity[slot]
            source = jnp.roll(post[slot], (vector[2], vector[1], vector[0]), axis=(0, 1, 2))
            open_cell = jnp.roll(fluid, (vector[2], vector[1], vector[0]), axis=(0, 1, 2))
            result.append(jnp.where(open_cell > 0.5, source, post[opposite[slot]]))
        fields = jnp.stack(result) * fluid[None]
    return fields
```

```python
import functools

import jax
import jax.numpy as jnp
from jax import lax
from jax.experimental import pallas as pl
from jax.experimental.pallas import tpu as pltpu
from jax.sharding import PartitionSpec as P

lattice_velocity = [
    (0, 0, 0),
    (1, 0, 0),
    (-1, 0, 0),
    (0, 1, 0),
    (0, -1, 0),
    (0, 0, 1),
    (0, 0, -1),
    (1, 1, 0),
    (-1, -1, 0),
    (1, -1, 0),
    (-1, 1, 0),
    (1, 0, 1),
    (-1, 0, -1),
    (1, 0, -1),
    (-1, 0, 1),
    (0, 1, 1),
    (0, -1, -1),
    (0, 1, -1),
    (0, -1, 1),
]
lattice_weights = [1.0 / 3.0] + [1.0 / 18.0] * 6 + [1.0 / 36.0] * 12
opposite = [0, 2, 1, 4, 3, 6, 5, 8, 7, 10, 9, 12, 11, 14, 13, 16, 15, 18, 17]
relax_time = 0.8
body_force = 0.005

Q = 19
NZ = 2
KZ = Q * NZ
ROWS = 8
LANES = 128
COLS = 256
GROUP = 8
NX = 4
MESH = pl.DeviceIdType.MESH
f32 = jnp.float32


def tree_sum(values):
    values = list(values)
    while len(values) > 1:
        values = [
            values[i] + values[i + 1] if i + 1 < len(values) else values[i]
            for i in range(0, len(values), 2)
        ]
    return values[0]


def collide(fields, fluid):
    mass = tree_sum(fields)
    inverse = 1.0 / jnp.where(fluid > 0.5, mass, 1.0)
    speeds = []
    for column in range(3):
        plus = tree_sum([fields[i] for i in range(Q) if lattice_velocity[i][column] > 0])
        minus = tree_sum([fields[i] for i in range(Q) if lattice_velocity[i][column] < 0])
        speeds.append((plus - minus) * inverse)
    speeds[2] = speeds[2] + relax_time * body_force
    square = speeds[0] * speeds[0] + speeds[1] * speeds[1] + speeds[2] * speeds[2]
    rest = 1.0 - 1.5 * square
    triple = [3.0 * s for s in speeds]
    keep = 1.0 - 1.0 / relax_time
    result = [None] * Q
    scaled = {w: mass * (w / relax_time) for w in sorted(set(lattice_weights))}
    result[0] = keep * fields[0] + scaled[lattice_weights[0]] * rest
    for slot in range(1, Q, 2):
        vector = lattice_velocity[slot]
        along = None
        for column in range(3):
            if vector[column]:
                if along is None:
                    along = triple[column] if vector[column] > 0 else -triple[column]
                else:
                    along = along + triple[column] if vector[column] > 0 else along - triple[column]
        weight = scaled[lattice_weights[slot]]
        even = weight * (rest + 0.5 * along * along)
        odd = weight * along
        other = opposite[slot]
        result[slot] = keep * fields[slot] + (even + odd)
        result[other] = keep * fields[other] + (even - odd)
    return result


def exchange_kernel(
    pop_ref, pore_ref, pen_ref, strip, voxel, relay, fold, halo, in_sem, give_sem, carry_sem,
    send_x, send_z, send_y, recv_y,
):
    px = lax.axis_index("px")
    py = lax.axis_index("py")
    count = lax.axis_size("py")
    zh = px // NX
    xx = px % NX
    partner = (1 - zh) * NX + xx
    up = lax.rem(py + 1, count)
    down = lax.rem(py + count - 1, count)

    def across(b):
        return zh * NX + lax.rem(xx + b, NX)

    barrier = pltpu.get_barrier_semaphore()
    for where in [(partner, py), (across(1), py), (across(2), py), (across(3), py), (px, up), (px, down)]:
        pl.semaphore_signal(barrier, inc=1, device_id=where, device_id_type=MESH)

    load_pop = pltpu.make_async_copy(pop_ref, strip.at[pl.ds(0, KZ)], in_sem.at[0])
    load_pore = pltpu.make_async_copy(pore_ref, voxel, in_sem.at[1])
    load_pop.start()
    load_pore.start()
    load_pore.wait()
    load_pop.wait()

    def collide_tile(j, carry):
        cols = pl.ds(pl.multiple_of(j * LANES, LANES), LANES)
        for z in range(NZ):
            fluid = voxel[z, :, cols].astype(f32)
            fields = [strip[i * NZ + z, :, cols] * fluid for i in range(Q)]
            post = collide(fields, fluid)
            for i in range(Q):
                strip[i * NZ + z, :, cols] = post[i]
        return carry

    width = strip.shape[2]
    lax.fori_loop(0, width // LANES, collide_tile, 0)

    lane = lax.broadcasted_iota(jnp.int32, (ROWS, LANES), 1)

    def pack_sides(p, carry):
        left = pl.ds(pl.multiple_of(lax.rem(p * COLS + width - LANES, width), LANES), LANES)
        right = pl.ds(pl.multiple_of(lax.rem(p * COLS + COLS, width), LANES), LANES)
        for tile in range(2):
            total = jnp.zeros((ROWS, LANES), f32)
            for k in range(tile * 32, min(KZ, tile * 32 + 32)):
                shift = 4 * (k % 32)
                side = jnp.where(lane < LANES // 2, strip[k, :, right], strip[k, :, left])
                if shift:
                    side = pltpu.roll(side, shift, 1)
                total = jnp.where(((lane - shift + 2) & (LANES - 1)) < 4, side, total)
            cols = pl.ds(pl.multiple_of(p * COLS + tile * LANES, LANES), LANES)
            strip[KZ, :, cols] = total
        return carry

    lax.fori_loop(0, GROUP, pack_sides, 0)

    def place(s):
        return pen_ref.at[:, pl.ds(pl.multiple_of(s * ROWS + ROWS, ROWS), ROWS), :]

    def piece(p):
        return strip.at[:, :, pl.ds(pl.multiple_of(p * COLS, COLS), COLS)]

    pl.semaphore_wait(barrier, 6)

    first = pltpu.make_async_remote_copy(
        src_ref=piece(partner), dst_ref=place(px), send_sem=send_z.at[0], recv_sem=give_sem.at[px],
        device_id=(partner, py), device_id_type=MESH)
    first.start()
    sends = [first]
    for b in (1, 3, 2):
        copy = pltpu.make_async_remote_copy(
            src_ref=piece((1 - zh) * NX + lax.rem(xx + b, NX)), dst_ref=relay.at[b - 1],
            send_sem=send_x.at[b - 1], recv_sem=carry_sem.at[b - 1],
            device_id=(across(b), py), device_id_type=MESH)
        copy.start()
        sends.append(copy)
    for b in (1, 3, 2):
        copy = pltpu.make_async_remote_copy(
            src_ref=piece(across(b)), dst_ref=place(px),
            send_sem=send_x.at[b + 2], recv_sem=give_sem.at[px],
            device_id=(across(b), py), device_id_type=MESH)
        copy.start()
        sends.append(copy)

    own = pl.ds(pl.multiple_of(px * COLS, COLS), COLS)
    mine = pl.ds(pl.multiple_of(px * ROWS + ROWS, ROWS), ROWS)

    def copy_own(k, carry):
        pen_ref[k, mine, :] = strip[k, :, own]
        return carry

    lax.fori_loop(0, KZ + 1, copy_own, 0)

    edge = lax.rem(xx + zh, NX)
    late = (edge == 2).astype(jnp.int32)
    for n, b in enumerate((1, 3 - late, 2 + late)):
        source = zh * NX + lax.rem(xx + NX - b, NX)
        arrival = pltpu.make_async_remote_copy(
            src_ref=relay.at[b - 1], dst_ref=relay.at[b - 1], send_sem=send_z.at[n + 1],
            recv_sem=carry_sem.at[b - 1], device_id=(partner, py), device_id_type=MESH)
        arrival.wait_recv()
        onward = pltpu.make_async_remote_copy(
            src_ref=relay.at[b - 1], dst_ref=place(source), send_sem=send_z.at[n + 1],
            recv_sem=give_sem.at[source], device_id=(partner, py), device_id_type=MESH)
        onward.start()
        sends.append(onward)

    def await_strip(s):
        @pl.when(px != s)
        def _():
            pltpu.make_async_remote_copy(
                src_ref=place(s), dst_ref=place(s), send_sem=send_z.at[0], recv_sem=give_sem.at[s],
                device_id=(partner, py), device_id_type=MESH).wait_recv()

    row = lax.broadcasted_iota(jnp.int32, (ROWS, COLS), 0)

    def pack_rows(side):
        block = pl.ds(GROUP * ROWS, ROWS) if side == 0 else pl.ds(ROWS, ROWS)
        for group in range(10):
            total = jnp.zeros((ROWS, COLS), f32)
            for j in range(4):
                k = group * 4 + j
                if k > KZ:
                    continue
                shift = (2 * j + (2 if side == 0 else 0)) % ROWS
                part = pen_ref[k, block, :]
                if shift:
                    part = pltpu.roll(part, shift, 0)
                total = jnp.where((row >> 1) == j, part, total)
            fold[side, group] = total

    ways = []
    for side, s in ((0, GROUP - 1), (1, 0)):
        await_strip(s)
        pack_rows(side)
        way = pltpu.make_async_remote_copy(
            src_ref=fold.at[side], dst_ref=halo.at[side], send_sem=send_y.at[side],
            recv_sem=recv_y.at[side], device_id=(px, up if side == 0 else down), device_id_type=MESH)
        way.start()
        ways.append(way)

    for side in range(2):
        ways[side].wait()
        block = pl.ds(0, ROWS) if side == 0 else pl.ds((GROUP + 1) * ROWS, ROWS)
        for k in range(KZ + 1):
            shift = (ROWS - 2 * (k % 4) - (2 if side == 0 else 0)) % ROWS
            part = halo[side, k // 4]
            if shift:
                part = pltpu.roll(part, shift, 0)
            pen_ref[k, block, :] = part

    for s in range(1, GROUP - 1):
        await_strip(s)
    for copy in sends:
        copy.wait_send()


def exchange(pop, pore):
    blocks = GROUP + 2
    return pl.pallas_call(
        exchange_kernel,
        out_shape=jax.ShapeDtypeStruct((KZ + 1, blocks * ROWS, COLS), f32),
        in_specs=[pl.BlockSpec(memory_space=pl.ANY)] * 2,
        out_specs=pl.BlockSpec(memory_space=pltpu.VMEM),
        scratch_shapes=[
            pltpu.VMEM((KZ + 1, ROWS, pop.shape[2]), f32),
            pltpu.VMEM(pore.shape, jnp.int32),
            pltpu.VMEM((3, KZ + 1, ROWS, COLS), f32),
            pltpu.VMEM((2, 10, ROWS, COLS), f32),
            pltpu.VMEM((2, 10, ROWS, COLS), f32),
            pltpu.SemaphoreType.DMA((2,)),
            pltpu.SemaphoreType.DMA((GROUP,)),
            pltpu.SemaphoreType.DMA((3,)),
            pltpu.SemaphoreType.DMA((6,)),
            pltpu.SemaphoreType.DMA((4,)),
            pltpu.SemaphoreType.DMA((2,)),
            pltpu.SemaphoreType.DMA((2,)),
        ],
        compiler_params=pltpu.CompilerParams(collective_id=0, has_side_effects=True),
        name="exchange",
    )(pop, pore)


def shifted(load, vector, lane, row):
    cx, cy = vector[0], vector[1]
    seam = LANES - 1 if cx > 0 else 0

    def along_x(dy):
        value = load(dy, 0)
        if cx:
            value = pltpu.roll(jnp.where(lane == seam, load(dy, -cx), value), cx % LANES, 1)
        return value

    value = along_x(0)
    if cy:
        edge = ROWS - 1 if cy > 0 else 0
        value = pltpu.roll(jnp.where(row == edge, along_x(-cy), value), cy % ROWS, 0)
    return value


def stream(load, load_fluid, z, lane, row):
    masks = {}
    fluid = load_fluid(z, 0, 0)
    result = []
    for slot in range(Q):
        vector = lattice_velocity[slot]
        if slot == 0:
            result.append(load(0, z, 0, 0) * fluid)
            continue
        plane = z ^ (vector[2] & 1)
        key = (vector[0], vector[1], plane)
        if key not in masks:
            masks[key] = shifted(functools.partial(load_fluid, plane), vector, lane, row) > 0.5
        source = shifted(functools.partial(load, slot, plane), vector, lane, row)
        result.append(jnp.where(masks[key], source, load(opposite[slot], z, 0, 0)) * fluid)
    return result, fluid


def steps_kernel(pen_ref, out_ref, side, open_ref, post, flow, out_sem):
    blocks = GROUP + 2
    lane = lax.broadcasted_iota(jnp.int32, (ROWS, LANES), 1)
    row = lax.broadcasted_iota(jnp.int32, (ROWS, LANES), 0)

    def rows_of(b):
        return pl.ds(pl.multiple_of(b * ROWS, ROWS), ROWS)

    def unfold(b, carry):
        rows = rows_of(b)
        for k in range(KZ):
            tile = k // 32
            part = pen_ref[KZ, rows, pl.ds(tile * LANES, LANES)]
            shift = -4 * (k % 32) % LANES
            side[k, rows, :] = pltpu.roll(part, shift, 1) if shift else part
        for z in range(NZ):
            mass = tree_sum([pen_ref[i * NZ + z, rows, :] for i in range(Q)])
            open_ref[z, rows, pl.ds(0, COLS)] = jnp.where(mass > 0.19, 1.0, 0.0)
            mass = tree_sum([side[i * NZ + z, rows, :] for i in range(Q)])
            open_ref[z, rows, pl.ds(COLS, LANES)] = jnp.where(mass > 0.19, 1.0, 0.0)
        return carry

    lax.fori_loop(0, blocks, unfold, 0)

    def near(b, dy):
        return rows_of(jnp.clip(b + dy, 0, blocks - 1)) if dy else rows_of(b)

    def first(b, carry):
        for tile in range(3):
            for z in range(NZ):

                def load(slot, plane, dy, dx):
                    t = (tile + dx) % 3
                    k = slot * NZ + plane
                    if t == 2:
                        return side[k, near(b, dy), :]
                    return pen_ref[k, near(b, dy), pl.ds(t * LANES, LANES)]

                def load_fluid(plane, dy, dx):
                    return open_ref[plane, near(b, dy), pl.ds((tile + dx) % 3 * LANES, LANES)]

                fields, fluid = stream(load, load_fluid, z, lane, row)
                for i, value in enumerate(collide(fields, fluid)):
                    post[i * NZ + z, rows_of(b), pl.ds(tile * LANES, LANES)] = value
        return carry

    lax.fori_loop(0, blocks, first, 0)

    def leave(b):
        return pltpu.make_async_copy(
            flow.at[:, pl.ds(pl.multiple_of((b - 1) * ROWS, ROWS), ROWS), :],
            out_ref.at[:, pl.ds(pl.multiple_of((b - 1) * ROWS, ROWS), ROWS), :],
            out_sem.at[b - 1])

    def second(b, carry):
        for tile in range(2):
            for z in range(NZ):

                def load(slot, plane, dy, dx):
                    return post[slot * NZ + plane, near(b, dy), pl.ds((tile + dx) % 3 * LANES, LANES)]

                def load_fluid(plane, dy, dx):
                    return open_ref[plane, near(b, dy), pl.ds((tile + dx) % 3 * LANES, LANES)]

                fields, _ = stream(load, load_fluid, z, lane, row)
                for i, value in enumerate(fields):
                    flow[i * NZ + z, pl.ds(pl.multiple_of((b - 1) * ROWS, ROWS), ROWS), pl.ds(tile * LANES, LANES)] = value
        leave(b).start()
        return carry

    lax.fori_loop(1, blocks - 1, second, 0)
    for b in range(1, blocks - 1):
        leave(b).wait()


def steps(pen):
    blocks = GROUP + 2
    return pl.pallas_call(
        steps_kernel,
        out_shape=jax.ShapeDtypeStruct((KZ, GROUP * ROWS, COLS), f32),
        in_specs=[pl.BlockSpec(memory_space=pltpu.VMEM)],
        out_specs=pl.BlockSpec(memory_space=pl.ANY),
        scratch_shapes=[
            pltpu.VMEM((KZ, blocks * ROWS, LANES), f32),
            pltpu.VMEM((NZ, blocks * ROWS, COLS + LANES), f32),
            pltpu.VMEM((KZ, blocks * ROWS, COLS + LANES), f32),
            pltpu.VMEM((KZ, GROUP * ROWS, COLS), f32),
            pltpu.SemaphoreType.DMA((GROUP,)),
        ],
        name="steps",
    )(pen)


def body(populations, pore):
    shape = populations.shape
    pen = exchange(populations.reshape(KZ, shape[2], shape[3]), pore)
    return steps(pen).reshape(Q, NZ, GROUP * ROWS, COLS)


def solution(mesh):
    return jax.shard_map(
        body,
        mesh=mesh,
        in_specs=(P(None, None, ("py", "px"), None), P(None, ("py", "px"), None)),
        out_specs=P(None, None, "py", "px"),
        check_vma=False,
    )
```

```python
import functools

import jax
import jax.numpy as jnp
from jax import lax
from jax.experimental import pallas as pl
from jax.experimental.pallas import tpu as pltpu
from jax.sharding import PartitionSpec as P

lattice_velocity = [
    (0, 0, 0),
    (1, 0, 0),
    (-1, 0, 0),
    (0, 1, 0),
    (0, -1, 0),
    (0, 0, 1),
    (0, 0, -1),
    (1, 1, 0),
    (-1, -1, 0),
    (1, -1, 0),
    (-1, 1, 0),
    (1, 0, 1),
    (-1, 0, -1),
    (1, 0, -1),
    (-1, 0, 1),
    (0, 1, 1),
    (0, -1, -1),
    (0, 1, -1),
    (0, -1, 1),
]
lattice_weights = [1.0 / 3.0] + [1.0 / 18.0] * 6 + [1.0 / 36.0] * 12
opposite = [0, 2, 1, 4, 3, 6, 5, 8, 7, 10, 9, 12, 11, 14, 13, 16, 15, 18, 17]
relax_time = 0.8
body_force = 0.005

Q = 19
NZ = 2
KZ = Q * NZ
ROWS = 8
LANES = 128
COLS = 256
GROUP = 8
NX = 4
MESH = pl.DeviceIdType.MESH
f32 = jnp.float32


def tree_sum(values):
    values = list(values)
    while len(values) > 1:
        values = [
            values[i] + values[i + 1] if i + 1 < len(values) else values[i]
            for i in range(0, len(values), 2)
        ]
    return values[0]


def collide(fields, fluid):
    mass = tree_sum(fields)
    inverse = 1.0 / jnp.where(fluid > 0.5, mass, 1.0)
    speeds = []
    for column in range(3):
        plus = tree_sum([fields[i] for i in range(Q) if lattice_velocity[i][column] > 0])
        minus = tree_sum([fields[i] for i in range(Q) if lattice_velocity[i][column] < 0])
        speeds.append((plus - minus) * inverse)
    speeds[2] = speeds[2] + relax_time * body_force
    square = speeds[0] * speeds[0] + speeds[1] * speeds[1] + speeds[2] * speeds[2]
    rest = 1.0 - 1.5 * square
    triple = [3.0 * s for s in speeds]
    keep = 1.0 - 1.0 / relax_time
    result = [None] * Q
    scaled = {w: mass * (w / relax_time) for w in sorted(set(lattice_weights))}
    result[0] = keep * fields[0] + scaled[lattice_weights[0]] * rest
    for slot in range(1, Q, 2):
        vector = lattice_velocity[slot]
        along = None
        for column in range(3):
            if vector[column]:
                if along is None:
                    along = triple[column] if vector[column] > 0 else -triple[column]
                else:
                    along = along + triple[column] if vector[column] > 0 else along - triple[column]
        weight = scaled[lattice_weights[slot]]
        even = weight * (rest + 0.5 * along * along)
        odd = weight * along
        other = opposite[slot]
        result[slot] = keep * fields[slot] + (even + odd)
        result[other] = keep * fields[other] + (even - odd)
    return result

BLOCKS = GROUP + 2
WIDE = COLS + LANES
WINDOW = 5
HALO_RANK = 4


def carried(px):
    late = (lax.rem(px % NX + px // NX, NX) == 2).astype(jnp.int32)
    return 1, 3 - late, 2 + late


def arrivals(px):
    xx = px % NX
    other = 1 - px // NX
    partner = other * NX + xx
    return (partner,) + tuple(other * NX + lax.rem(xx + NX - b, NX) for b in carried(partner))


def rows_of(b):
    return pl.ds(pl.multiple_of(b * ROWS, ROWS), ROWS)


def near(b, dy):
    return rows_of(jnp.clip(b + dy, 0, BLOCKS - 1)) if dy else rows_of(b)


def second_step(post_ref, open_ref, flow_ref, b, at, lane, row):
    for tile in range(2):

        def load(slot, plane, dy, dx):
            return post_ref[slot * NZ + plane, near(b, dy), pl.ds((tile + dx) % 3 * LANES, LANES)]

        def load_fluid(plane, dy, dx):
            return open_ref[plane, near(b, dy), pl.ds((tile + dx) % 3 * LANES, LANES)]

        for z in range(NZ):
            fields, _ = stream(load, load_fluid, z, lane, row)
            for i, value in enumerate(fields):
                flow_ref[i * NZ + z, at, pl.ds(tile * LANES, LANES)] = value


def shifted(load, vector, lane, row):
    cx, cy = vector[0], vector[1]
    seam = LANES - 1 if cx > 0 else 0

    def along_x(dy):
        value = load(dy, 0)
        if cx:
            value = pltpu.roll(jnp.where(lane == seam, load(dy, -cx), value), cx % LANES, 1)
        return value

    value = along_x(0)
    if cy:
        edge = ROWS - 1 if cy > 0 else 0
        value = pltpu.roll(jnp.where(row == edge, along_x(-cy), value), cy % ROWS, 0)
    return value


def stream(load, load_fluid, z, lane, row):
    masks = {}
    fluid = load_fluid(z, 0, 0)
    result = []
    for slot in range(Q):
        vector = lattice_velocity[slot]
        if slot == 0:
            result.append(load(0, z, 0, 0) * fluid)
            continue
        plane = z ^ (vector[2] & 1)
        key = (vector[0], vector[1], plane)
        if key not in masks:
            masks[key] = shifted(functools.partial(load_fluid, plane), vector, lane, row) > 0.5
        source = shifted(functools.partial(load, slot, plane), vector, lane, row)
        result.append(jnp.where(masks[key], source, load(opposite[slot], z, 0, 0)) * fluid)
    return result, fluid


def exchange_kernel(
    pop_ref, pore_ref, post_ref, open_ref, flow_ref, early, raw, voxel, strip, relay, fold, halo, pen, side,
    in_sem, give_sem, carry_sem, send_x, send_z, send_y, recv_y,
):
    px = lax.axis_index("px")
    py = lax.axis_index("py")
    count = lax.axis_size("py")
    zh = px // NX
    xx = px % NX
    partner = (1 - zh) * NX + xx
    up = lax.rem(py + 1, count)
    down = lax.rem(py + count - 1, count)

    def across(b):
        return zh * NX + lax.rem(xx + b, NX)

    barrier = pltpu.get_barrier_semaphore()
    for where in [(partner, py), (across(1), py), (across(2), py), (across(3), py), (px, up), (px, down)]:
        pl.semaphore_signal(barrier, inc=1, device_id=where, device_id_type=MESH)

    width = strip.shape[2]
    tiles = width // LANES

    def tile_at(t):
        return pl.ds(pl.multiple_of(lax.rem(t, tiles) * LANES, LANES), LANES)

    home = partner * 2 + tiles - 1
    loads = [
        pltpu.make_async_copy(pore_ref, voxel, in_sem.at[0]),
        pltpu.make_async_copy(pop_ref.at[:, :, tile_at(home)], early.at[:, :, pl.ds(0, LANES)], in_sem.at[1]),
        pltpu.make_async_copy(
            pop_ref.at[:, :, pl.ds(pl.multiple_of(partner * COLS, COLS), COLS)],
            early.at[:, :, pl.ds(LANES, COLS)], in_sem.at[2]),
        pltpu.make_async_copy(
            pop_ref.at[:, :, tile_at(home + 3)], early.at[:, :, pl.ds(LANES + COLS, LANES)], in_sem.at[3]),
        pltpu.make_async_copy(pop_ref, raw, in_sem.at[4]),
    ]
    for load in loads:
        load.start()

    lane = lax.broadcasted_iota(jnp.int32, (ROWS, LANES), 1)
    row = lax.broadcasted_iota(jnp.int32, (ROWS, LANES), 0)

    def collide_tile(source, cols, to):
        for z in range(NZ):
            fluid = voxel[z, :, to].astype(f32)
            fields = [source[i * NZ + z, :, cols] * fluid for i in range(Q)]
            for i, value in enumerate(collide(fields, fluid)):
                strip[i * NZ + z, :, to] = value

    def pack_sides(p):
        left = tile_at(p * 2 + tiles - 1)
        right = tile_at(p * 2 + 2)
        for tile in range(2):
            total = jnp.zeros((ROWS, LANES), f32)
            for k in range(tile * 32, min(KZ, tile * 32 + 32)):
                turn = 4 * (k % 32)
                part = jnp.where(lane < LANES // 2, strip[k, :, right], strip[k, :, left])
                if turn:
                    part = pltpu.roll(part, turn, 1)
                total = jnp.where(((lane - turn + 2) & (LANES - 1)) < 4, part, total)
            strip[KZ, :, tile_at(p * 2 + tile)] = total

    def early_tile(t, carry):
        collide_tile(early, pl.ds(pl.multiple_of(t * LANES, LANES), LANES), tile_at(home + t))
        return carry

    def late_tile(t, carry):
        collide_tile(raw, tile_at(home + t), tile_at(home + t))
        return carry

    def late_sides(n, carry):
        pack_sides(lax.rem(partner + n, GROUP))
        return carry

    def place(s):
        return pen.at[:, rows_of(s + 1), :]

    def piece(p):
        return strip.at[:, :, pl.ds(pl.multiple_of(p * COLS, COLS), COLS)]

    for load in loads[:4]:
        load.wait()
    lax.fori_loop(0, 4, early_tile, 0)
    pack_sides(partner)
    pl.semaphore_wait(barrier, 6)

    first = pltpu.make_async_remote_copy(
        src_ref=piece(partner), dst_ref=place(px), send_sem=send_z.at[0], recv_sem=give_sem.at[px],
        device_id=(partner, py), device_id_type=MESH)
    first.start()
    sends = [first]

    loads[4].wait()
    lax.fori_loop(4, tiles, late_tile, 0)
    lax.fori_loop(1, GROUP, late_sides, 0)

    order = (1, 3, 2)
    for n, b in enumerate(order):
        copy = pltpu.make_async_remote_copy(
            src_ref=piece((1 - zh) * NX + lax.rem(xx + b, NX)), dst_ref=relay.at[b - 1],
            send_sem=send_x.at[n], recv_sem=carry_sem.at[b - 1],
            device_id=(across(b), py), device_id_type=MESH)
        copy.start()
        sends.append(copy)
    for n, b in enumerate(order):
        copy = pltpu.make_async_remote_copy(
            src_ref=piece(across(b)), dst_ref=place(px),
            send_sem=send_x.at[n + 3], recv_sem=give_sem.at[px],
            device_id=(across(b), py), device_id_type=MESH)
        copy.start()
        sends.append(copy)

    own = pl.ds(pl.multiple_of(px * COLS, COLS), COLS)
    mine = rows_of(px + 1)

    def copy_own(k, carry):
        pen[k, mine, :] = strip[k, :, own]
        return carry

    lax.fori_loop(0, KZ + 1, copy_own, 0)

    for n, b in enumerate(carried(px)):
        source = zh * NX + lax.rem(xx + NX - b, NX)
        arrival = pltpu.make_async_remote_copy(
            src_ref=relay.at[b - 1], dst_ref=relay.at[b - 1], send_sem=send_z.at[n + 1],
            recv_sem=carry_sem.at[b - 1], device_id=(partner, py), device_id_type=MESH)
        arrival.wait_recv()
        onward = pltpu.make_async_remote_copy(
            src_ref=relay.at[b - 1], dst_ref=place(source), send_sem=send_z.at[n + 1],
            recv_sem=give_sem.at[source], device_id=(partner, py), device_id_type=MESH)
        onward.start()
        sends.append(onward)

    def await_strip(s):
        pltpu.make_async_remote_copy(
            src_ref=place(s), dst_ref=place(s), send_sem=send_z.at[0], recv_sem=give_sem.at[s],
            device_id=(partner, py), device_id_type=MESH).wait_recv()

    wide_row = lax.broadcasted_iota(jnp.int32, (ROWS, COLS), 0)

    def pack_rows(way):
        block = pl.ds(GROUP * ROWS, ROWS) if way == 0 else pl.ds(ROWS, ROWS)
        for group in range(10):
            total = jnp.zeros((ROWS, COLS), f32)
            for j in range(4):
                k = group * 4 + j
                if k > KZ:
                    continue
                turn = (2 * j + (2 if way == 0 else 0)) % ROWS
                part = pen[k, block, :]
                if turn:
                    part = pltpu.roll(part, turn, 0)
                total = jnp.where((wide_row >> 1) == j, part, total)
            fold[way, group] = total

    def unfold(b):
        rows = rows_of(b)
        for k in range(KZ):
            part = pen[KZ, rows, pl.ds(k // 32 * LANES, LANES)]
            turn = -4 * (k % 32) % LANES
            side[k, rows, :] = pltpu.roll(part, turn, 1) if turn else part
        for z in range(NZ):
            mass = tree_sum([pen[i * NZ + z, rows, :] for i in range(Q)])
            open_ref[z, rows, pl.ds(0, COLS)] = jnp.where(mass > 0.19, 1.0, 0.0)
            mass = tree_sum([side[i * NZ + z, rows, :] for i in range(Q)])
            open_ref[z, rows, pl.ds(COLS, LANES)] = jnp.where(mass > 0.19, 1.0, 0.0)

    def first_step(b):
        for tile in range(3):

            def load(slot, plane, dy, dx):
                t = (tile + dx) % 3
                k = slot * NZ + plane
                if t == 2:
                    return side[k, near(b, dy), :]
                return pen[k, near(b, dy), pl.ds(t * LANES, LANES)]

            def load_fluid(plane, dy, dx):
                return open_ref[plane, near(b, dy), pl.ds((tile + dx) % 3 * LANES, LANES)]

            for z in range(NZ):
                fields, fluid = stream(load, load_fluid, z, lane, row)
                for i, value in enumerate(collide(fields, fluid)):
                    post_ref[i * NZ + z, rows_of(b), pl.ds(tile * LANES, LANES)] = value

    coming = arrivals(px)
    last = coming[3]
    begin = jnp.clip(last - 2, 0, GROUP - WINDOW)

    def rank(b):
        s = b - 1
        late = jnp.where(s == last, 5, 3)
        for n in (2, 1, 0):
            late = jnp.where(s == coming[n], n + 1, late)
        late = jnp.where(s // NX == zh, 0, late)
        return jnp.where(jnp.logical_or(b <= 0, b >= BLOCKS - 1), HALO_RANK, late)

    def stage(n):
        def unfold_some(b, carry):
            @pl.when(rank(b) == n)
            def _():
                unfold(b)
            return carry

        def first_some(b, carry):
            @pl.when(jnp.maximum(jnp.maximum(rank(b - 1), rank(b)), rank(b + 1)) == n)
            def _():
                first_step(b)
            return carry

        lax.fori_loop(1, BLOCKS - 1, unfold_some, 0)
        lax.fori_loop(0, BLOCKS, first_some, 0)

    def half(n, carry):
        s = zh * NX + n

        @pl.when(s != px)
        def _():
            await_strip(s)
        return carry

    lax.fori_loop(0, NX, half, 0)
    stage(0)
    await_strip(coming[0])
    stage(1)
    await_strip(coming[1])
    stage(2)
    await_strip(coming[2])
    ways = []
    for way in range(2):
        pack_rows(way)
        copy = pltpu.make_async_remote_copy(
            src_ref=fold.at[way], dst_ref=halo.at[way], send_sem=send_y.at[way],
            recv_sem=recv_y.at[way], device_id=(px, up if way == 0 else down), device_id_type=MESH)
        copy.start()
        ways.append(copy)
    stage(3)
    for way in range(2):
        ways[way].wait()
        block = pl.ds(0, ROWS) if way == 0 else pl.ds((GROUP + 1) * ROWS, ROWS)
        for k in range(KZ + 1):
            turn = (ROWS - 2 * (k % 4) - (2 if way == 0 else 0)) % ROWS
            part = halo[way, k // 4]
            if turn:
                part = pltpu.roll(part, turn, 0)
            pen[k, block, :] = part
    unfold(0)
    unfold(BLOCKS - 1)
    stage(HALO_RANK)

    def second_come(n, carry):
        s = lax.rem(begin + WINDOW + n, GROUP)
        second_step(post_ref, open_ref, flow_ref, s + 1, rows_of(s), lane, row)
        return carry

    lax.fori_loop(0, GROUP - WINDOW, second_come, 0)
    await_strip(last)
    unfold(last + 1)

    def first_rest(b, carry):
        first_step(b)
        return carry

    lax.fori_loop(last, last + 3, first_rest, 0)
    for copy in sends:
        copy.wait_send()


def exchange(pop, pore):
    return pl.pallas_call(
        exchange_kernel,
        out_shape=[
            pltpu.VMEM((KZ, BLOCKS * ROWS, WIDE), f32),
            pltpu.VMEM((NZ, BLOCKS * ROWS, WIDE), f32),
            pltpu.VMEM((KZ, GROUP * ROWS, COLS), f32),
        ],
        in_specs=[pl.BlockSpec(memory_space=pltpu.HBM)] * 2,
        out_specs=[pl.BlockSpec(memory_space=pltpu.VMEM)] * 3,
        scratch_shapes=[
            pltpu.VMEM((KZ, ROWS, COLS + 2 * LANES), f32),
            pltpu.VMEM((KZ, ROWS, pop.shape[2]), f32),
            pltpu.VMEM(pore.shape, jnp.int32),
            pltpu.VMEM((KZ + 1, ROWS, pop.shape[2]), f32),
            pltpu.VMEM((3, KZ + 1, ROWS, COLS), f32),
            pltpu.VMEM((2, 10, ROWS, COLS), f32),
            pltpu.VMEM((2, 10, ROWS, COLS), f32),
            pltpu.VMEM((KZ + 1, BLOCKS * ROWS, COLS), f32),
            pltpu.VMEM((KZ, BLOCKS * ROWS, LANES), f32),
            pltpu.SemaphoreType.DMA((5,)),
            pltpu.SemaphoreType.DMA((GROUP,)),
            pltpu.SemaphoreType.DMA((3,)),
            pltpu.SemaphoreType.DMA((6,)),
            pltpu.SemaphoreType.DMA((4,)),
            pltpu.SemaphoreType.DMA((2,)),
            pltpu.SemaphoreType.DMA((2,)),
        ],
        compiler_params=pltpu.CompilerParams(collective_id=0, has_side_effects=True, vmem_limit_bytes=40 * 2**20),
        name="exchange",
    )(pltpu.with_memory_space_constraint(pop, pltpu.HBM), pltpu.with_memory_space_constraint(pore, pltpu.HBM))


def finish_kernel(post_ref, open_ref, flow_ref, out_ref, rest, out_sem):
    lane = lax.broadcasted_iota(jnp.int32, (ROWS, LANES), 1)
    row = lax.broadcasted_iota(jnp.int32, (ROWS, LANES), 0)
    last = arrivals(lax.axis_index("px"))[3]
    begin = jnp.clip(last - 2, 0, GROUP - WINDOW)

    def ready(n):
        s = lax.rem(begin + WINDOW + n, GROUP)
        return pltpu.make_async_copy(flow_ref.at[:, rows_of(s), :], out_ref.at[:, rows_of(s), :], out_sem.at[n + WINDOW])

    def fresh(n):
        return pltpu.make_async_copy(rest.at[:, rows_of(n), :], out_ref.at[:, rows_of(begin + n), :], out_sem.at[n])

    for n in range(GROUP - WINDOW):
        ready(n).start()

    def second_rest(n, carry):
        second_step(post_ref, open_ref, rest, begin + n + 1, rows_of(n), lane, row)
        fresh(n).start()
        return carry

    lax.fori_loop(0, WINDOW, second_rest, 0)
    for n in range(GROUP - WINDOW):
        ready(n).wait()
    for n in range(WINDOW):
        fresh(n).wait()


def finish(post, opened, flow):
    return pl.pallas_call(
        finish_kernel,
        out_shape=jax.ShapeDtypeStruct(flow.shape, f32),
        in_specs=[pl.BlockSpec(memory_space=pltpu.VMEM)] * 3,
        out_specs=pl.BlockSpec(memory_space=pl.ANY),
        scratch_shapes=[
            pltpu.VMEM((KZ, WINDOW * ROWS, COLS), f32),
            pltpu.SemaphoreType.DMA((GROUP,)),
        ],
        compiler_params=pltpu.CompilerParams(vmem_limit_bytes=24 * 2**20),
        name="finish",
    )(post, opened, flow)


def body(populations, pore):
    shape = populations.shape
    parts = exchange(populations.reshape(KZ, shape[2], shape[3]), pore)
    return finish(*parts).reshape(Q, NZ, GROUP * ROWS, COLS)


def solution(mesh):
    return jax.shard_map(
        body,
        mesh=mesh,
        in_specs=(P(None, None, ("py", "px"), None), P(None, ("py", "px"), None)),
        out_specs=P(None, None, "py", "px"),
        check_vma=False,
    )
```

```python
import functools

import jax
import jax.numpy as jnp
from jax import lax
from jax.experimental import pallas as pl
from jax.experimental.pallas import tpu as pltpu
from jax.sharding import PartitionSpec as P

lattice_velocity = [
    (0, 0, 0),
    (1, 0, 0),
    (-1, 0, 0),
    (0, 1, 0),
    (0, -1, 0),
    (0, 0, 1),
    (0, 0, -1),
    (1, 1, 0),
    (-1, -1, 0),
    (1, -1, 0),
    (-1, 1, 0),
    (1, 0, 1),
    (-1, 0, -1),
    (1, 0, -1),
    (-1, 0, 1),
    (0, 1, 1),
    (0, -1, -1),
    (0, 1, -1),
    (0, -1, 1),
]
lattice_weights = [1.0 / 3.0] + [1.0 / 18.0] * 6 + [1.0 / 36.0] * 12
opposite = [0, 2, 1, 4, 3, 6, 5, 8, 7, 10, 9, 12, 11, 14, 13, 16, 15, 18, 17]
relax_time = 0.8
body_force = 0.005

Q = 19
NZ = 2
KZ = Q * NZ
ROWS = 8
LANES = 128
COLS = 256
GROUP = 8
NX = 4
MESH = pl.DeviceIdType.MESH
f32 = jnp.float32


def tree_sum(values):
    values = list(values)
    while len(values) > 1:
        values = [
            values[i] + values[i + 1] if i + 1 < len(values) else values[i]
            for i in range(0, len(values), 2)
        ]
    return values[0]


def collide(fields, fluid):
    mass = tree_sum(fields)
    inverse = 1.0 / jnp.where(fluid > 0.5, mass, 1.0)
    speeds = []
    for column in range(3):
        plus = tree_sum([fields[i] for i in range(Q) if lattice_velocity[i][column] > 0])
        minus = tree_sum([fields[i] for i in range(Q) if lattice_velocity[i][column] < 0])
        speeds.append((plus - minus) * inverse)
    speeds[2] = speeds[2] + relax_time * body_force
    square = speeds[0] * speeds[0] + speeds[1] * speeds[1] + speeds[2] * speeds[2]
    rest = 1.0 - 1.5 * square
    triple = [3.0 * s for s in speeds]
    keep = 1.0 - 1.0 / relax_time
    result = [None] * Q
    scaled = {w: mass * (w / relax_time) for w in sorted(set(lattice_weights))}
    result[0] = keep * fields[0] + scaled[lattice_weights[0]] * rest
    for slot in range(1, Q, 2):
        vector = lattice_velocity[slot]
        along = None
        for column in range(3):
            if vector[column]:
                if along is None:
                    along = triple[column] if vector[column] > 0 else -triple[column]
                else:
                    along = along + triple[column] if vector[column] > 0 else along - triple[column]
        weight = scaled[lattice_weights[slot]]
        even = weight * (rest + 0.5 * along * along)
        odd = weight * along
        other = opposite[slot]
        result[slot] = keep * fields[slot] + (even + odd)
        result[other] = keep * fields[other] + (even - odd)
    return result

BLOCKS = GROUP + 1
WIDE = COLS + LANES
WINDOW = 5
FRONT = 20
HALO_RANK = 4


def carried(px):
    edge = lax.rem(px % NX + px // NX, NX)
    first = 1 + 2 * (edge == 3).astype(jnp.int32)
    final = 2 + (edge == 2).astype(jnp.int32)
    return first, 6 - first - final, final


def arrivals(px):
    xx = px % NX
    other = 1 - px // NX
    partner = other * NX + xx
    return (partner,) + tuple(other * NX + lax.rem(xx + NX - b, NX) for b in carried(partner))


def rows_of(b):
    return pl.ds(pl.multiple_of(b * ROWS, ROWS), ROWS)


def near(b, dy):
    return rows_of(lax.rem(b + dy + BLOCKS, BLOCKS)) if dy else rows_of(b)


def second_step(post_ref, open_ref, flow_ref, b, at, lane, row):
    for tile in range(2):

        def load(slot, plane, dy, dx):
            return post_ref[slot * NZ + plane, near(b, dy), pl.ds((tile + dx) % 3 * LANES, LANES)]

        def load_fluid(plane, dy, dx):
            return open_ref[plane, near(b, dy), pl.ds((tile + dx) % 3 * LANES, LANES)]

        for z in range(NZ):
            fields, _ = stream(load, load_fluid, z, lane, row)
            for i, value in enumerate(fields):
                flow_ref[i * NZ + z, at, pl.ds(tile * LANES, LANES)] = value


def shifted(load, vector, lane, row):
    cx, cy = vector[0], vector[1]
    seam = LANES - 1 if cx > 0 else 0

    def along_x(dy):
        value = load(dy, 0)
        if cx:
            value = pltpu.roll(jnp.where(lane == seam, load(dy, -cx), value), cx % LANES, 1)
        return value

    value = along_x(0)
    if cy:
        edge = ROWS - 1 if cy > 0 else 0
        value = pltpu.roll(jnp.where(row == edge, along_x(-cy), value), cy % ROWS, 0)
    return value


def stream(load, load_fluid, z, lane, row):
    masks = {}
    fluid = load_fluid(z, 0, 0)
    result = []
    for slot in range(Q):
        vector = lattice_velocity[slot]
        if slot == 0:
            result.append(load(0, z, 0, 0) * fluid)
            continue
        plane = z ^ (vector[2] & 1)
        key = (vector[0], vector[1], plane)
        if key not in masks:
            masks[key] = shifted(functools.partial(load_fluid, plane), vector, lane, row) > 0.5
        source = shifted(functools.partial(load, slot, plane), vector, lane, row)
        result.append(jnp.where(masks[key], source, load(opposite[slot], z, 0, 0)) * fluid)
    return result, fluid


def exchange_kernel(
    pop_ref, pore_ref, post_ref, open_ref, flow_ref, early, raw, voxel, strip, relay, fold, halo, pen, side,
    in_sem, give_sem, carry_sem, send_x, send_z, send_y, recv_y,
):
    px = lax.axis_index("px")
    py = lax.axis_index("py")
    count = lax.axis_size("py")
    zh = px // NX
    xx = px % NX
    partner = (1 - zh) * NX + xx
    up = lax.rem(py + 1, count)
    down = lax.rem(py + count - 1, count)

    def across(b):
        return zh * NX + lax.rem(xx + b, NX)

    barrier = pltpu.get_barrier_semaphore()
    for where in [(partner, py), (across(1), py), (across(2), py), (across(3), py), (px, up), (px, down)]:
        pl.semaphore_signal(barrier, inc=1, device_id=where, device_id_type=MESH)

    width = strip.shape[2]
    tiles = width // LANES

    def tile_at(t):
        return pl.ds(pl.multiple_of(lax.rem(t, tiles) * LANES, LANES), LANES)

    home = partner * 2 + tiles - 1
    loads = [
        pltpu.make_async_copy(pore_ref, voxel, in_sem.at[0]),
        pltpu.make_async_copy(pop_ref.at[:, :, tile_at(home)], early.at[:, :, pl.ds(0, LANES)], in_sem.at[1]),
        pltpu.make_async_copy(
            pop_ref.at[:, :, pl.ds(pl.multiple_of(partner * COLS, COLS), COLS)],
            early.at[:, :, pl.ds(LANES, COLS)], in_sem.at[2]),
        pltpu.make_async_copy(
            pop_ref.at[:, :, tile_at(home + 3)], early.at[:, :, pl.ds(LANES + COLS, LANES)], in_sem.at[3]),
        pltpu.make_async_copy(pop_ref, raw, in_sem.at[4]),
    ]
    for load in loads:
        load.start()

    lane = lax.broadcasted_iota(jnp.int32, (ROWS, LANES), 1)
    row = lax.broadcasted_iota(jnp.int32, (ROWS, LANES), 0)

    def collide_tile(source, cols, to):
        for z in range(NZ):
            fluid = voxel[z, :, to].astype(f32)
            fields = [source[i * NZ + z, :, cols] * fluid for i in range(Q)]
            for i, value in enumerate(collide(fields, fluid)):
                strip[i * NZ + z, :, to] = value

    def pack_sides(p):
        left = tile_at(p * 2 + tiles - 1)
        right = tile_at(p * 2 + 2)
        for tile in range(2):
            total = jnp.zeros((ROWS, LANES), f32)
            for k in range(tile * 32, min(KZ, tile * 32 + 32)):
                turn = 4 * (k % 32)
                part = jnp.where(lane < LANES // 2, strip[k, :, right], strip[k, :, left])
                if turn:
                    part = pltpu.roll(part, turn, 1)
                total = jnp.where(((lane - turn + 2) & (LANES - 1)) < 4, part, total)
            strip[KZ, :, tile_at(p * 2 + tile)] = total

    def early_tile(t, carry):
        collide_tile(early, pl.ds(pl.multiple_of(t * LANES, LANES), LANES), tile_at(home + t))
        return carry

    def late_tile(t, carry):
        collide_tile(raw, tile_at(home + t), tile_at(home + t))
        return carry

    def late_sides(n, carry):
        pack_sides(lax.rem(partner + n, GROUP))
        return carry

    def place(s):
        return pen.at[:, rows_of(s + 1), :]

    def piece(p):
        return strip.at[:, :, pl.ds(pl.multiple_of(p * COLS, COLS), COLS)]

    for load in loads[:4]:
        load.wait()
    lax.fori_loop(0, 4, early_tile, 0)
    pack_sides(partner)
    pl.semaphore_wait(barrier, 6)

    first = pltpu.make_async_remote_copy(
        src_ref=piece(partner), dst_ref=place(px), send_sem=send_z.at[0], recv_sem=give_sem.at[px],
        device_id=(partner, py), device_id_type=MESH)
    first.start()
    sends = [first]

    loads[4].wait()
    lax.fori_loop(4, tiles, late_tile, 0)
    lax.fori_loop(1, GROUP, late_sides, 0)

    order = (1, 3, 2)
    for n, b in enumerate(order):
        copy = pltpu.make_async_remote_copy(
            src_ref=piece((1 - zh) * NX + lax.rem(xx + b, NX)), dst_ref=relay.at[b - 1],
            send_sem=send_x.at[n], recv_sem=carry_sem.at[b - 1],
            device_id=(across(b), py), device_id_type=MESH)
        copy.start()
        sends.append(copy)
    own = pl.ds(pl.multiple_of(px * COLS, COLS), COLS)
    mine = rows_of(px + 1)

    def copy_own(k, carry):
        pen[k, mine, :] = strip[k, :, own]
        return carry

    lax.fori_loop(0, KZ + 1, copy_own, 0)

    def carry_on(n, b, parts):
        source = zh * NX + lax.rem(xx + NX - b, NX)
        pltpu.make_async_remote_copy(
            src_ref=relay.at[b - 1], dst_ref=relay.at[b - 1], send_sem=send_z.at[n],
            recv_sem=carry_sem.at[b - 1], device_id=(partner, py), device_id_type=MESH).wait_recv()
        return [
            pltpu.make_async_remote_copy(
                src_ref=relay.at[b - 1, planes], dst_ref=pen.at[planes, rows_of(source + 1), :],
                send_sem=send_z.at[n + m], recv_sem=give_sem.at[source if m == 0 else GROUP],
                device_id=(partner, py), device_id_type=MESH)
            for m, planes in enumerate(parts)
        ]

    whole = [pl.ds(0, KZ + 1)]
    halves = [pl.ds(0, FRONT), pl.ds(FRONT, KZ + 1 - FRONT)]
    turns = carried(px)
    for n in range(2):
        onward = carry_on(n + 1, turns[n], whole)
        onward[0].start()
        sends += onward
    final = carry_on(3, turns[2], halves)
    sends += final

    for n, b in enumerate(order):
        copy = pltpu.make_async_remote_copy(
            src_ref=piece(across(b)), dst_ref=place(px),
            send_sem=send_x.at[n + 3], recv_sem=give_sem.at[px],
            device_id=(across(b), py), device_id_type=MESH)
        copy.start()
        sends.append(copy)

    def await_strip(s):
        pltpu.make_async_remote_copy(
            src_ref=place(s), dst_ref=place(s), send_sem=send_z.at[0], recv_sem=give_sem.at[s],
            device_id=(partner, py), device_id_type=MESH).wait_recv()

    def await_last(s):
        for m, planes in enumerate(halves):
            part = pen.at[planes, rows_of(s + 1), :]
            pltpu.make_async_remote_copy(
                src_ref=part, dst_ref=part, send_sem=send_z.at[0], recv_sem=give_sem.at[s if m == 0 else GROUP],
                device_id=(partner, py), device_id_type=MESH).wait_recv()

    wide_row = lax.broadcasted_iota(jnp.int32, (ROWS, COLS), 0)

    def pack_rows(way):
        block = pl.ds(GROUP * ROWS, ROWS) if way == 0 else pl.ds(ROWS, ROWS)
        for group in range(10):
            total = jnp.zeros((ROWS, COLS), f32)
            for j in range(4):
                k = group * 4 + j
                if k > KZ:
                    continue
                turn = (2 * j + (2 if way == 0 else 0)) % ROWS
                part = pen[k, block, :]
                if turn:
                    part = pltpu.roll(part, turn, 0)
                total = jnp.where((wide_row >> 1) == j, part, total)
            fold[way, group] = total

    def unfold(b):
        rows = rows_of(b)
        for k in range(KZ):
            part = pen[KZ, rows, pl.ds(k // 32 * LANES, LANES)]
            turn = -4 * (k % 32) % LANES
            side[k, rows, :] = pltpu.roll(part, turn, 1) if turn else part
        for z in range(NZ):
            mass = tree_sum([pen[i * NZ + z, rows, :] for i in range(Q)])
            open_ref[z, rows, pl.ds(0, COLS)] = jnp.where(mass > 0.19, 1.0, 0.0)
            mass = tree_sum([side[i * NZ + z, rows, :] for i in range(Q)])
            open_ref[z, rows, pl.ds(COLS, LANES)] = jnp.where(mass > 0.19, 1.0, 0.0)

    def first_step(b):
        for tile in range(3):

            def load(slot, plane, dy, dx):
                t = (tile + dx) % 3
                k = slot * NZ + plane
                if t == 2:
                    return side[k, near(b, dy), :]
                return pen[k, near(b, dy), pl.ds(t * LANES, LANES)]

            def load_fluid(plane, dy, dx):
                return open_ref[plane, near(b, dy), pl.ds((tile + dx) % 3 * LANES, LANES)]

            for z in range(NZ):
                fields, fluid = stream(load, load_fluid, z, lane, row)
                for i, value in enumerate(collide(fields, fluid)):
                    post_ref[i * NZ + z, rows_of(b), pl.ds(tile * LANES, LANES)] = value

    coming = arrivals(px)
    last = coming[3]
    begin = jnp.clip(last - 2, 0, GROUP - WINDOW)

    def rank(block):
        b = lax.rem(block + BLOCKS, BLOCKS)
        s = b - 1
        late = jnp.where(s == last, 5, 3)
        for n in (2, 1, 0):
            late = jnp.where(s == coming[n], n + 1, late)
        late = jnp.where(s // NX == zh, 0, late)
        return jnp.where(b == 0, HALO_RANK, late)

    def stage(n):
        def unfold_some(b, carry):
            @pl.when(rank(b) == n)
            def _():
                unfold(b)
            return carry

        def first_some(b, carry):
            @pl.when(jnp.maximum(jnp.maximum(rank(b - 1), rank(b)), rank(b + 1)) == n)
            def _():
                first_step(b)
            return carry

        lax.fori_loop(1, BLOCKS, unfold_some, 0)
        lax.fori_loop(0, BLOCKS, first_some, 0)

    def half(n, carry):
        s = zh * NX + n

        @pl.when(s != px)
        def _():
            await_strip(s)
        return carry

    ways = [
        pltpu.make_async_remote_copy(
            src_ref=fold.at[way], dst_ref=halo.at[way], send_sem=send_y.at[way], recv_sem=recv_y.at[way],
            device_id=(px, up if way == 0 else down), device_id_type=MESH)
        for way in range(2)
    ]
    def hand_on(early):
        for way in range(2):
            @pl.when((zh + way == 1) == early)
            def _():
                pack_rows(way)
                ways[way].start()

    lax.fori_loop(0, NX, half, 0)
    hand_on(True)
    stage(0)
    await_strip(coming[0])
    stage(1)
    await_strip(coming[1])
    final[0].start()
    def take_over():
        for way in range(2):
            ways[way].wait()
        for k in range(KZ + 1):
            parts = []
            for way in range(2):
                turn = (ROWS - 2 * (k % 4) - (2 if way == 0 else 0)) % ROWS
                part = halo[way, k // 4]
                parts.append(pltpu.roll(part, turn, 0) if turn else part)
            pen[k, pl.ds(0, ROWS), :] = jnp.where(wide_row < ROWS // 2, parts[1], parts[0])
        unfold(0)

    stage(2)
    await_strip(coming[2])
    hand_on(False)
    final[1].start()
    stage(3)
    take_over()
    stage(HALO_RANK)

    def second_come(n, carry):
        s = lax.rem(begin + WINDOW + n, GROUP)
        second_step(post_ref, open_ref, flow_ref, s + 1, rows_of(s), lane, row)
        return carry

    lax.fori_loop(0, GROUP - WINDOW, second_come, 0)
    await_last(last)
    unfold(last + 1)

    def first_rest(b, carry):
        first_step(b)
        return carry

    lax.fori_loop(last, last + 3, first_rest, 0)
    for copy in sends:
        copy.wait_send()


def exchange(pop, pore):
    return pl.pallas_call(
        exchange_kernel,
        out_shape=[
            pltpu.VMEM((KZ, BLOCKS * ROWS, WIDE), f32),
            pltpu.VMEM((NZ, BLOCKS * ROWS, WIDE), f32),
            pltpu.VMEM((KZ, GROUP * ROWS, COLS), f32),
        ],
        in_specs=[pl.BlockSpec(memory_space=pltpu.HBM)] * 2,
        out_specs=[pl.BlockSpec(memory_space=pltpu.VMEM)] * 3,
        scratch_shapes=[
            pltpu.VMEM((KZ, ROWS, COLS + 2 * LANES), f32),
            pltpu.VMEM((KZ, ROWS, pop.shape[2]), f32),
            pltpu.VMEM(pore.shape, jnp.int32),
            pltpu.VMEM((KZ + 1, ROWS, pop.shape[2]), f32),
            pltpu.VMEM((3, KZ + 1, ROWS, COLS), f32),
            pltpu.VMEM((2, 10, ROWS, COLS), f32),
            pltpu.VMEM((2, 10, ROWS, COLS), f32),
            pltpu.VMEM((KZ + 1, BLOCKS * ROWS, COLS), f32),
            pltpu.VMEM((KZ, BLOCKS * ROWS, LANES), f32),
            pltpu.SemaphoreType.DMA((5,)),
            pltpu.SemaphoreType.DMA((GROUP + 1,)),
            pltpu.SemaphoreType.DMA((3,)),
            pltpu.SemaphoreType.DMA((6,)),
            pltpu.SemaphoreType.DMA((5,)),
            pltpu.SemaphoreType.DMA((2,)),
            pltpu.SemaphoreType.DMA((2,)),
        ],
        compiler_params=pltpu.CompilerParams(collective_id=0, has_side_effects=True, vmem_limit_bytes=40 * 2**20),
        name="exchange",
    )(pltpu.with_memory_space_constraint(pop, pltpu.HBM), pltpu.with_memory_space_constraint(pore, pltpu.HBM))


def finish_kernel(post_ref, open_ref, flow_ref, out_ref, rest, out_sem):
    lane = lax.broadcasted_iota(jnp.int32, (ROWS, LANES), 1)
    row = lax.broadcasted_iota(jnp.int32, (ROWS, LANES), 0)
    last = arrivals(lax.axis_index("px"))[3]
    begin = jnp.clip(last - 2, 0, GROUP - WINDOW)

    def ready(n):
        s = lax.rem(begin + WINDOW + n, GROUP)
        return pltpu.make_async_copy(flow_ref.at[:, rows_of(s), :], out_ref.at[:, rows_of(s), :], out_sem.at[n + WINDOW])

    def fresh(n):
        return pltpu.make_async_copy(rest.at[:, rows_of(n), :], out_ref.at[:, rows_of(begin + n), :], out_sem.at[n])

    for n in range(GROUP - WINDOW):
        ready(n).start()

    def second_rest(n, carry):
        second_step(post_ref, open_ref, rest, begin + n + 1, rows_of(n), lane, row)
        fresh(n).start()
        return carry

    lax.fori_loop(0, WINDOW, second_rest, 0)
    for n in range(GROUP - WINDOW):
        ready(n).wait()
    for n in range(WINDOW):
        fresh(n).wait()


def finish(post, opened, flow):
    return pl.pallas_call(
        finish_kernel,
        out_shape=jax.ShapeDtypeStruct(flow.shape, f32),
        in_specs=[pl.BlockSpec(memory_space=pltpu.VMEM)] * 3,
        out_specs=pl.BlockSpec(memory_space=pl.ANY),
        scratch_shapes=[
            pltpu.VMEM((KZ, WINDOW * ROWS, COLS), f32),
            pltpu.SemaphoreType.DMA((GROUP,)),
        ],
        compiler_params=pltpu.CompilerParams(vmem_limit_bytes=24 * 2**20),
        name="finish",
    )(post, opened, flow)


def body(populations, pore):
    shape = populations.shape
    parts = exchange(populations.reshape(KZ, shape[2], shape[3]), pore)
    return finish(*parts).reshape(Q, NZ, GROUP * ROWS, COLS)


def solution(mesh):
    return jax.shard_map(
        body,
        mesh=mesh,
        in_specs=(P(None, None, ("py", "px"), None), P(None, ("py", "px"), None)),
        out_specs=P(None, None, "py", "px"),
        check_vma=False,
    )
```

```python
import functools

import jax
import jax.numpy as jnp
from jax import lax
from jax.experimental import pallas as pl
from jax.experimental.pallas import tpu as pltpu
from jax.sharding import PartitionSpec as P

lattice_velocity = [
    (0, 0, 0),
    (1, 0, 0),
    (-1, 0, 0),
    (0, 1, 0),
    (0, -1, 0),
    (0, 0, 1),
    (0, 0, -1),
    (1, 1, 0),
    (-1, -1, 0),
    (1, -1, 0),
    (-1, 1, 0),
    (1, 0, 1),
    (-1, 0, -1),
    (1, 0, -1),
    (-1, 0, 1),
    (0, 1, 1),
    (0, -1, -1),
    (0, 1, -1),
    (0, -1, 1),
]
lattice_weights = [1.0 / 3.0] + [1.0 / 18.0] * 6 + [1.0 / 36.0] * 12
opposite = [0, 2, 1, 4, 3, 6, 5, 8, 7, 10, 9, 12, 11, 14, 13, 16, 15, 18, 17]
relax_time = 0.8
body_force = 0.005

Q = 19
NZ = 2
KZ = Q * NZ
ROWS = 8
LANES = 128
COLS = 256
GROUP = 8
NX = 4
MESH = pl.DeviceIdType.MESH
f32 = jnp.float32


def tree_sum(values):
    values = list(values)
    while len(values) > 1:
        values = [
            values[i] + values[i + 1] if i + 1 < len(values) else values[i]
            for i in range(0, len(values), 2)
        ]
    return values[0]


def collide(fields, fluid):
    mass = tree_sum(fields)
    inverse = 1.0 / jnp.where(fluid > 0.5, mass, 1.0)
    speeds = []
    for column in range(3):
        plus = tree_sum([fields[i] for i in range(Q) if lattice_velocity[i][column] > 0])
        minus = tree_sum([fields[i] for i in range(Q) if lattice_velocity[i][column] < 0])
        speeds.append((plus - minus) * inverse)
    speeds[2] = speeds[2] + relax_time * body_force
    square = speeds[0] * speeds[0] + speeds[1] * speeds[1] + speeds[2] * speeds[2]
    rest = 1.0 - 1.5 * square
    triple = [3.0 * s for s in speeds]
    keep = 1.0 - 1.0 / relax_time
    result = [None] * Q
    scaled = {w: mass * (w / relax_time) for w in sorted(set(lattice_weights))}
    result[0] = keep * fields[0] + scaled[lattice_weights[0]] * rest
    for slot in range(1, Q, 2):
        vector = lattice_velocity[slot]
        along = None
        for column in range(3):
            if vector[column]:
                if along is None:
                    along = triple[column] if vector[column] > 0 else -triple[column]
                else:
                    along = along + triple[column] if vector[column] > 0 else along - triple[column]
        weight = scaled[lattice_weights[slot]]
        even = weight * (rest + 0.5 * along * along)
        odd = weight * along
        other = opposite[slot]
        result[slot] = keep * fields[slot] + (even + odd)
        result[other] = keep * fields[other] + (even - odd)
    return result

BLOCKS = GROUP + 1
WIDE = COLS + LANES
WINDOW = 5
FRONT = 20
HALO_RANK = 4


def carried(px):
    edge = lax.rem(px % NX + px // NX, NX)
    first = 1 + 2 * (edge == 3).astype(jnp.int32)
    final = 2 + (edge == 2).astype(jnp.int32)
    return first, 6 - first - final, final


def arrivals(px):
    xx = px % NX
    other = 1 - px // NX
    partner = other * NX + xx
    return (partner,) + tuple(other * NX + lax.rem(xx + NX - b, NX) for b in carried(partner))


def rows_of(b):
    return pl.ds(pl.multiple_of(b * ROWS, ROWS), ROWS)


def near(b, dy):
    return rows_of(lax.rem(b + dy + BLOCKS, BLOCKS)) if dy else rows_of(b)


def second_step(post_ref, open_ref, flow_ref, b, at, lane, row):
    for tile in range(2):

        def load(slot, plane, dy, dx):
            return post_ref[slot * NZ + plane, near(b, dy), pl.ds((tile + dx) % 3 * LANES, LANES)]

        def load_fluid(plane, dy, dx):
            return open_ref[plane, near(b, dy), pl.ds((tile + dx) % 3 * LANES, LANES)]

        for z in range(NZ):
            fields, _ = stream(load, load_fluid, z, lane, row)
            for i, value in enumerate(fields):
                flow_ref[i * NZ + z, at, pl.ds(tile * LANES, LANES)] = value


def shifted(load, vector, lane, row):
    cx, cy = vector[0], vector[1]
    seam = LANES - 1 if cx > 0 else 0

    def along_x(dy):
        value = load(dy, 0)
        if cx:
            value = pltpu.roll(jnp.where(lane == seam, load(dy, -cx), value), cx % LANES, 1)
        return value

    value = along_x(0)
    if cy:
        edge = ROWS - 1 if cy > 0 else 0
        value = pltpu.roll(jnp.where(row == edge, along_x(-cy), value), cy % ROWS, 0)
    return value


def stream(load, load_fluid, z, lane, row):
    masks = {}
    fluid = load_fluid(z, 0, 0)
    result = []
    for slot in range(Q):
        vector = lattice_velocity[slot]
        if slot == 0:
            result.append(load(0, z, 0, 0) * fluid)
            continue
        plane = z ^ (vector[2] & 1)
        key = (vector[0], vector[1], plane)
        if key not in masks:
            masks[key] = shifted(functools.partial(load_fluid, plane), vector, lane, row) > 0.5
        source = shifted(functools.partial(load, slot, plane), vector, lane, row)
        result.append(jnp.where(masks[key], source, load(opposite[slot], z, 0, 0)) * fluid)
    return result, fluid


def exchange_kernel(
    pop_ref, pore_ref, post_ref, open_ref, flow_ref, early, raw, voxel, strip, relay, fold, halo, pen, side,
    in_sem, give_sem, carry_sem, send_x, send_z, send_y, recv_y,
):
    px = lax.axis_index("px")
    py = lax.axis_index("py")
    count = lax.axis_size("py")
    zh = px // NX
    xx = px % NX
    partner = (1 - zh) * NX + xx
    up = lax.rem(py + 1, count)
    down = lax.rem(py + count - 1, count)

    def across(b):
        return zh * NX + lax.rem(xx + b, NX)

    barrier = pltpu.get_barrier_semaphore()
    for where in [(partner, py), (across(1), py), (across(2), py), (across(3), py), (px, up), (px, down)]:
        pl.semaphore_signal(barrier, inc=1, device_id=where, device_id_type=MESH)

    width = strip.shape[2]
    tiles = width // LANES

    def tile_at(t):
        return pl.ds(pl.multiple_of(lax.rem(t, tiles) * LANES, LANES), LANES)

    home = partner * 2 + tiles - 1
    loads = [
        pltpu.make_async_copy(pore_ref, voxel, in_sem.at[0]),
        pltpu.make_async_copy(pop_ref.at[:, :, tile_at(home)], early.at[:, :, pl.ds(0, LANES)], in_sem.at[1]),
        pltpu.make_async_copy(
            pop_ref.at[:, :, pl.ds(pl.multiple_of(partner * COLS, COLS), COLS)],
            early.at[:, :, pl.ds(LANES, COLS)], in_sem.at[2]),
        pltpu.make_async_copy(
            pop_ref.at[:, :, tile_at(home + 3)], early.at[:, :, pl.ds(LANES + COLS, LANES)], in_sem.at[3]),
        pltpu.make_async_copy(pop_ref, raw, in_sem.at[4]),
    ]
    for load in loads:
        load.start()

    lane = lax.broadcasted_iota(jnp.int32, (ROWS, LANES), 1)
    row = lax.broadcasted_iota(jnp.int32, (ROWS, LANES), 0)

    def collide_tile(source, cols, to):
        for z in range(NZ):
            fluid = voxel[z, :, to].astype(f32)
            fields = [source[i * NZ + z, :, cols] * fluid for i in range(Q)]
            for i, value in enumerate(collide(fields, fluid)):
                strip[i * NZ + z, :, to] = value

    def pack_sides(p):
        left = tile_at(p * 2 + tiles - 1)
        right = tile_at(p * 2 + 2)
        for tile in range(2):
            total = jnp.zeros((ROWS, LANES), f32)
            for k in range(tile * 32, min(KZ, tile * 32 + 32)):
                turn = 4 * (k % 32)
                part = jnp.where(lane < LANES // 2, strip[k, :, right], strip[k, :, left])
                if turn:
                    part = pltpu.roll(part, turn, 1)
                total = jnp.where(((lane - turn + 2) & (LANES - 1)) < 4, part, total)
            strip[KZ, :, tile_at(p * 2 + tile)] = total

    def early_tile(t, carry):
        collide_tile(early, pl.ds(pl.multiple_of(t * LANES, LANES), LANES), tile_at(home + t))
        return carry

    def late_tile(t, carry):
        collide_tile(raw, tile_at(home + t), tile_at(home + t))
        return carry

    def late_sides(n, carry):
        pack_sides(lax.rem(partner + n, GROUP))
        return carry

    def place(s):
        return pen.at[:, rows_of(s + 1), :]

    def piece(p):
        return strip.at[:, :, pl.ds(pl.multiple_of(p * COLS, COLS), COLS)]

    loads[0].wait()
    loads[2].wait()
    lax.fori_loop(1, 3, early_tile, 0)
    pl.semaphore_wait(barrier, 6)

    opening = [
        pltpu.make_async_remote_copy(
            src_ref=piece(partner).at[planes], dst_ref=place(px).at[planes], send_sem=send_z.at[5 * m],
            recv_sem=give_sem.at[px if m == 0 else GROUP + 1], device_id=(partner, py), device_id_type=MESH)
        for m, planes in enumerate((pl.ds(0, KZ), pl.ds(KZ, 1)))
    ]
    opening[0].start()
    loads[1].wait()
    loads[3].wait()
    early_tile(0, 0)
    early_tile(3, 0)
    pack_sides(partner)
    opening[1].start()
    sends = list(opening)

    loads[4].wait()
    lax.fori_loop(4, tiles, late_tile, 0)
    lax.fori_loop(1, GROUP, late_sides, 0)

    order = (1, 3, 2)
    for n, b in enumerate(order):
        copy = pltpu.make_async_remote_copy(
            src_ref=piece((1 - zh) * NX + lax.rem(xx + b, NX)), dst_ref=relay.at[b - 1],
            send_sem=send_x.at[n], recv_sem=carry_sem.at[b - 1],
            device_id=(across(b), py), device_id_type=MESH)
        copy.start()
        sends.append(copy)
    own = pl.ds(pl.multiple_of(px * COLS, COLS), COLS)
    mine = rows_of(px + 1)

    def copy_own(k, carry):
        pen[k, mine, :] = strip[k, :, own]
        return carry

    lax.fori_loop(0, KZ + 1, copy_own, 0)

    def carry_on(n, b, parts):
        source = zh * NX + lax.rem(xx + NX - b, NX)
        pltpu.make_async_remote_copy(
            src_ref=relay.at[b - 1], dst_ref=relay.at[b - 1], send_sem=send_z.at[n],
            recv_sem=carry_sem.at[b - 1], device_id=(partner, py), device_id_type=MESH).wait_recv()
        return [
            pltpu.make_async_remote_copy(
                src_ref=relay.at[b - 1, planes], dst_ref=pen.at[planes, rows_of(source + 1), :],
                send_sem=send_z.at[n + m], recv_sem=give_sem.at[source if m == 0 else GROUP],
                device_id=(partner, py), device_id_type=MESH)
            for m, planes in enumerate(parts)
        ]

    whole = [pl.ds(0, KZ + 1)]
    halves = [pl.ds(0, FRONT), pl.ds(FRONT, KZ + 1 - FRONT)]
    turns = carried(px)
    for n in range(2):
        onward = carry_on(n + 1, turns[n], whole)
        onward[0].start()
        sends += onward
    final = carry_on(3, turns[2], halves)
    sends += final

    for n, b in enumerate(order):
        copy = pltpu.make_async_remote_copy(
            src_ref=piece(across(b)), dst_ref=place(px),
            send_sem=send_x.at[n + 3], recv_sem=give_sem.at[px],
            device_id=(across(b), py), device_id_type=MESH)
        copy.start()
        sends.append(copy)

    def await_strip(s):
        pltpu.make_async_remote_copy(
            src_ref=place(s), dst_ref=place(s), send_sem=send_z.at[0], recv_sem=give_sem.at[s],
            device_id=(partner, py), device_id_type=MESH).wait_recv()

    def await_opening(s):
        for m, planes in enumerate((pl.ds(0, KZ), pl.ds(KZ, 1))):
            part = place(s).at[planes]
            pltpu.make_async_remote_copy(
                src_ref=part, dst_ref=part, send_sem=send_z.at[0], recv_sem=give_sem.at[s if m == 0 else GROUP + 1],
                device_id=(partner, py), device_id_type=MESH).wait_recv()

    def await_last(s):
        for m, planes in enumerate(halves):
            part = pen.at[planes, rows_of(s + 1), :]
            pltpu.make_async_remote_copy(
                src_ref=part, dst_ref=part, send_sem=send_z.at[0], recv_sem=give_sem.at[s if m == 0 else GROUP],
                device_id=(partner, py), device_id_type=MESH).wait_recv()

    wide_row = lax.broadcasted_iota(jnp.int32, (ROWS, COLS), 0)

    def pack_rows(way):
        block = pl.ds(GROUP * ROWS, ROWS) if way == 0 else pl.ds(ROWS, ROWS)
        for group in range(10):
            total = jnp.zeros((ROWS, COLS), f32)
            for j in range(4):
                k = group * 4 + j
                if k > KZ:
                    continue
                turn = (2 * j + (2 if way == 0 else 0)) % ROWS
                part = pen[k, block, :]
                if turn:
                    part = pltpu.roll(part, turn, 0)
                total = jnp.where((wide_row >> 1) == j, part, total)
            fold[way, group] = total

    def unfold(b):
        rows = rows_of(b)
        for k in range(KZ):
            part = pen[KZ, rows, pl.ds(k // 32 * LANES, LANES)]
            turn = -4 * (k % 32) % LANES
            side[k, rows, :] = pltpu.roll(part, turn, 1) if turn else part
        for z in range(NZ):
            mass = tree_sum([pen[i * NZ + z, rows, :] for i in range(Q)])
            open_ref[z, rows, pl.ds(0, COLS)] = jnp.where(mass > 0.19, 1.0, 0.0)
            mass = tree_sum([side[i * NZ + z, rows, :] for i in range(Q)])
            open_ref[z, rows, pl.ds(COLS, LANES)] = jnp.where(mass > 0.19, 1.0, 0.0)

    def first_step(b):
        for tile in range(3):

            def load(slot, plane, dy, dx):
                t = (tile + dx) % 3
                k = slot * NZ + plane
                if t == 2:
                    return side[k, near(b, dy), :]
                return pen[k, near(b, dy), pl.ds(t * LANES, LANES)]

            def load_fluid(plane, dy, dx):
                return open_ref[plane, near(b, dy), pl.ds((tile + dx) % 3 * LANES, LANES)]

            for z in range(NZ):
                fields, fluid = stream(load, load_fluid, z, lane, row)
                for i, value in enumerate(collide(fields, fluid)):
                    post_ref[i * NZ + z, rows_of(b), pl.ds(tile * LANES, LANES)] = value

    coming = arrivals(px)
    last = coming[3]
    begin = jnp.clip(last - 2, 0, GROUP - WINDOW)

    def rank(block):
        b = lax.rem(block + BLOCKS, BLOCKS)
        s = b - 1
        late = jnp.where(s == last, 5, 3)
        for n in (2, 1, 0):
            late = jnp.where(s == coming[n], n + 1, late)
        late = jnp.where(s // NX == zh, 0, late)
        return jnp.where(b == 0, HALO_RANK, late)

    def stage(n):
        def unfold_some(b, carry):
            @pl.when(rank(b) == n)
            def _():
                unfold(b)
            return carry

        def first_some(b, carry):
            @pl.when(jnp.maximum(jnp.maximum(rank(b - 1), rank(b)), rank(b + 1)) == n)
            def _():
                first_step(b)
            return carry

        lax.fori_loop(1, BLOCKS, unfold_some, 0)
        lax.fori_loop(0, BLOCKS, first_some, 0)

    def half(n, carry):
        s = zh * NX + n

        @pl.when(s != px)
        def _():
            await_strip(s)
        return carry

    ways = [
        pltpu.make_async_remote_copy(
            src_ref=fold.at[way], dst_ref=halo.at[way], send_sem=send_y.at[way], recv_sem=recv_y.at[way],
            device_id=(px, up if way == 0 else down), device_id_type=MESH)
        for way in range(2)
    ]
    def hand_on(early):
        for way in range(2):
            @pl.when((zh + way == 1) == early)
            def _():
                pack_rows(way)
                ways[way].start()

    lax.fori_loop(0, NX, half, 0)
    hand_on(True)
    stage(0)
    await_opening(coming[0])
    stage(1)
    await_strip(coming[1])
    soon = lax.rem(partner % NX + partner // NX, NX) < 2

    @pl.when(soon)
    def _():
        hand_on(False)

    final[0].start()
    def take_over():
        for way in range(2):
            ways[way].wait()
        for k in range(KZ + 1):
            parts = []
            for way in range(2):
                turn = (ROWS - 2 * (k % 4) - (2 if way == 0 else 0)) % ROWS
                part = halo[way, k // 4]
                parts.append(pltpu.roll(part, turn, 0) if turn else part)
            pen[k, pl.ds(0, ROWS), :] = jnp.where(wide_row < ROWS // 2, parts[1], parts[0])
        unfold(0)

    stage(2)
    await_strip(coming[2])

    @pl.when(jnp.logical_not(soon))
    def _():
        hand_on(False)

    final[1].start()
    stage(3)
    take_over()
    stage(HALO_RANK)

    def second_come(n, carry):
        s = lax.rem(begin + WINDOW + n, GROUP)
        second_step(post_ref, open_ref, flow_ref, s + 1, rows_of(s), lane, row)
        return carry

    lax.fori_loop(0, GROUP - WINDOW, second_come, 0)
    await_last(last)
    unfold(last + 1)

    def first_rest(b, carry):
        first_step(b)
        return carry

    lax.fori_loop(last, last + 3, first_rest, 0)
    for copy in sends:
        copy.wait_send()


def exchange(pop, pore):
    return pl.pallas_call(
        exchange_kernel,
        out_shape=[
            pltpu.VMEM((KZ, BLOCKS * ROWS, WIDE), f32),
            pltpu.VMEM((NZ, BLOCKS * ROWS, WIDE), f32),
            pltpu.VMEM((KZ, GROUP * ROWS, COLS), f32),
        ],
        in_specs=[pl.BlockSpec(memory_space=pltpu.HBM)] * 2,
        out_specs=[pl.BlockSpec(memory_space=pltpu.VMEM)] * 3,
        scratch_shapes=[
            pltpu.VMEM((KZ, ROWS, COLS + 2 * LANES), f32),
            pltpu.VMEM((KZ, ROWS, pop.shape[2]), f32),
            pltpu.VMEM(pore.shape, jnp.int32),
            pltpu.VMEM((KZ + 1, ROWS, pop.shape[2]), f32),
            pltpu.VMEM((3, KZ + 1, ROWS, COLS), f32),
            pltpu.VMEM((2, 10, ROWS, COLS), f32),
            pltpu.VMEM((2, 10, ROWS, COLS), f32),
            pltpu.VMEM((KZ + 1, BLOCKS * ROWS, COLS), f32),
            pltpu.VMEM((KZ, BLOCKS * ROWS, LANES), f32),
            pltpu.SemaphoreType.DMA((5,)),
            pltpu.SemaphoreType.DMA((GROUP + 2,)),
            pltpu.SemaphoreType.DMA((3,)),
            pltpu.SemaphoreType.DMA((6,)),
            pltpu.SemaphoreType.DMA((6,)),
            pltpu.SemaphoreType.DMA((2,)),
            pltpu.SemaphoreType.DMA((2,)),
        ],
        compiler_params=pltpu.CompilerParams(collective_id=0, has_side_effects=True, vmem_limit_bytes=40 * 2**20),
        name="exchange",
    )(pltpu.with_memory_space_constraint(pop, pltpu.HBM), pltpu.with_memory_space_constraint(pore, pltpu.HBM))


def finish_kernel(post_ref, open_ref, flow_ref, out_ref, rest, out_sem):
    lane = lax.broadcasted_iota(jnp.int32, (ROWS, LANES), 1)
    row = lax.broadcasted_iota(jnp.int32, (ROWS, LANES), 0)
    last = arrivals(lax.axis_index("px"))[3]
    begin = jnp.clip(last - 2, 0, GROUP - WINDOW)

    def ready(n):
        s = lax.rem(begin + WINDOW + n, GROUP)
        return pltpu.make_async_copy(flow_ref.at[:, rows_of(s), :], out_ref.at[:, rows_of(s), :], out_sem.at[n + WINDOW])

    def fresh(n):
        return pltpu.make_async_copy(rest.at[:, rows_of(n), :], out_ref.at[:, rows_of(begin + n), :], out_sem.at[n])

    for n in range(GROUP - WINDOW):
        ready(n).start()

    def second_rest(n, carry):
        second_step(post_ref, open_ref, rest, begin + n + 1, rows_of(n), lane, row)
        fresh(n).start()
        return carry

    lax.fori_loop(0, WINDOW, second_rest, 0)
    for n in range(GROUP - WINDOW):
        ready(n).wait()
    for n in range(WINDOW):
        fresh(n).wait()


def finish(post, opened, flow):
    return pl.pallas_call(
        finish_kernel,
        out_shape=jax.ShapeDtypeStruct(flow.shape, f32),
        in_specs=[pl.BlockSpec(memory_space=pltpu.VMEM)] * 3,
        out_specs=pl.BlockSpec(memory_space=pl.ANY),
        scratch_shapes=[
            pltpu.VMEM((KZ, WINDOW * ROWS, COLS), f32),
            pltpu.SemaphoreType.DMA((GROUP,)),
        ],
        compiler_params=pltpu.CompilerParams(vmem_limit_bytes=24 * 2**20),
        name="finish",
    )(post, opened, flow)


def body(populations, pore):
    shape = populations.shape
    parts = exchange(populations.reshape(KZ, shape[2], shape[3]), pore)
    return finish(*parts).reshape(Q, NZ, GROUP * ROWS, COLS)


def solution(mesh):
    return jax.shard_map(
        body,
        mesh=mesh,
        in_specs=(P(None, None, ("py", "px"), None), P(None, ("py", "px"), None)),
        out_specs=P(None, None, "py", "px"),
        check_vma=False,
    )
```
